128 devices in a mesh: win: 2 (over core), grp: 64 (over z, y, x).
Axes of the slice: x: 4, y: 4, z: 4, core: 2. Of those that a mesh axis runs over, the one named last changes fastest.
Arguments:
- atom_table: float32 [4, 6, 98304], P('win', None, 'grp'), as said below
- row_blocks: int32 [4, 4096], P('win', 'grp'), may hold values from 0 to 767, as said below
- col_blocks: int32 [4, 4096], P('win', 'grp'), may hold values from 0 to 767, as said below
- lambdas: float32 [4], replicated, may hold values from 0 to 1, as said below
- inverse_temp: float32 [1], replicated, may hold values from 20 to 80
- parity: int32 [1], replicated, may hold values from 0 to 1073741823
- thresholds: int32 [4], replicated, may hold values from 0 to 1073741823
Outputs:
- energies: float32 [4, 3], P('win')
- margins: float32 [4], P('win')
- profile: float32 [4], P('win')
The draws below stay inside these ranges and needn't reach their ends.
Inputs may be any that keep to these rules, and one draw needn't show every extreme that they name: `row_blocks`: the first block of each pair listed on index g of grp lies in that index's share of atoms: blocks g * 12 to (g + 1) * 12 - 1. `col_blocks`: the list of one index of grp names blocks of any one index of grp (itself included) at most 2 times; in each window some index of grp has exactly 2 of its blocks named in every list of that window. `lambdas`: strictly increasing. `atom_table`: field 4 lies in 0.7 to 1.4 and field 5 in 0.6 to 1.4.
All inputs are finite; a program needn't handle non-finite values.
Results may differ from the reference program's by a relative error of at most 0.0003.
Values sent between devices are 32-bit elements; how exact they have to be, the bound alone decides.
A program may use at most 64 MiB of HBM per device.

```python
import math
import jax
import jax.numpy as jnp
from jax import lax

TILE = 128
BLK_DEV = 12
PB_DEV = 64
WINDOWS = 4
BLOCKS = 768
ATOMS = 98304
PAIRS = 4096
SLOTS = 2


def draw_atom_table(key, part):
    keys = jax.random.split(key, 12)
    regions = BLOCKS // BLK_DEV
    centres = jax.random.uniform(keys[0], (WINDOWS, 3, BLOCKS, 1), minval=-1.5, maxval=1.5)
    radius = jnp.exp(jax.random.uniform(keys[1], (WINDOWS, 1, BLOCKS, 1), minval=jnp.log(0.25), maxval=jnp.log(0.9)))
    offsets = jax.random.normal(keys[2], (WINDOWS, 3, BLOCKS, TILE))
    region_charge = 0.3 + 0.6 * jax.random.normal(keys[3], (WINDOWS, regions))
    block_charge = 0.3 * jax.random.normal(keys[4], (WINDOWS, BLOCKS))
    atom_charge = 0.3 * jax.random.normal(keys[5], (WINDOWS, BLOCKS, TILE))
    coords = (centres + radius * offsets).reshape(WINDOWS, 3, ATOMS)
    charge_block = jnp.repeat(region_charge, BLK_DEV, axis=1) + block_charge
    charge = (charge_block[:, :, None] + atom_charge).reshape(WINDOWS, 1, ATOMS)
    depth_block = jnp.exp(jax.random.uniform(keys[6], (WINDOWS, BLOCKS, 1), minval=jnp.log(0.75), maxval=jnp.log(1.3)))
    depth_atom = jnp.exp(jax.random.uniform(keys[7], (WINDOWS, BLOCKS, TILE), minval=jnp.log(0.935), maxval=jnp.log(1.07)))
    depth_root = (depth_block * depth_atom).reshape(WINDOWS, 1, ATOMS)
    size_block = jax.random.uniform(keys[8], (WINDOWS, BLOCKS, 1), minval=0.65, maxval=1.35)
    size_atom = jax.random.uniform(keys[9], (WINDOWS, BLOCKS, TILE), minval=-0.05, maxval=0.05)
    size_sq = (size_block + size_atom).reshape(WINDOWS, 1, ATOMS)
    return jnp.concatenate([coords, charge, depth_root, size_sq], axis=1).astype(jnp.float32)


def draw_row_blocks(key, part):
    offset = jnp.arange(PAIRS, dtype=jnp.int32) // PB_DEV * BLK_DEV
    picks = jax.random.randint(key, (WINDOWS, PAIRS), 0, BLK_DEV, dtype=jnp.int32)
    return picks + offset[None, :]


def draw_col_blocks(key, part):
    groups = PAIRS // PB_DEV
    pool = jnp.arange(groups * SLOTS, dtype=jnp.int32) // SLOTS
    keys = jax.random.split(jax.random.fold_in(key, 7), 2)
    heavy = jax.random.randint(keys[0], (WINDOWS,), 0, groups, dtype=jnp.int32)
    list_keys = jax.random.split(keys[1], WINDOWS * groups)

    def one_list(list_key, heavy_owner):
        first_key, second_key, third_key = jax.random.split(list_key, 3)
        order = jax.random.permutation(first_key, groups * SLOTS)
        owners = pool[order]
        placed = jnp.argsort((owners != heavy_owner).astype(jnp.int32), stable=True)
        chosen = owners[placed][:PB_DEV]
        chosen = jax.random.permutation(second_key, chosen)
        within = jax.random.randint(third_key, (PB_DEV,), 0, BLK_DEV, dtype=jnp.int32)
        return (chosen * BLK_DEV + within).astype(jnp.int32)
    heavy_rows = jnp.repeat(heavy, groups)
    lists = jax.vmap(one_list)(list_keys, heavy_rows)
    return lists.reshape(WINDOWS, PAIRS).astype(jnp.int32)


def draw_lambdas(key, part):
    keys = jax.random.split(jax.random.fold_in(key, 11), 3)
    increments = jax.random.uniform(keys[0], (WINDOWS,), minval=0.5, maxval=1.5)
    start = jax.random.uniform(keys[1], (), minval=0.0, maxval=0.25)
    finish = jax.random.uniform(keys[2], (), minval=0.75, maxval=1.0)
    running = jnp.cumsum(increments)
    unit = (running - running[0]) / (running[-1] - running[0])
    return (start + (finish - start) * unit).astype(jnp.float32)


def plant(drawn, key, least, largest):
    extent = drawn.shape
    place = [jax.random.randint(jax.random.fold_in(key, axis), (), 0, extent[axis]) for axis in range(len(extent))]
    drawn = drawn.at[tuple(place)].set(least)
    longest = extent.index(max(extent))
    place[longest] = (place[longest] + 1) % extent[longest]
    return drawn.at[tuple(place)].set(largest)


def setup_inputs(seed: int = 0) -> dict:
    seeds = jax.random.split(jax.random.key(seed), 8)
    return {
        "atom_table": draw_atom_table(jax.random.fold_in(seeds[7], 71), 0),
        "row_blocks": draw_row_blocks(jax.random.fold_in(seeds[7], 71), 0),
        "col_blocks": draw_col_blocks(jax.random.fold_in(seeds[7], 71), 0),
        "lambdas": draw_lambdas(jax.random.fold_in(seeds[7], 71), 0),
        "inverse_temp": jnp.clip(jnp.exp(jax.random.uniform(seeds[4], (1,), jnp.float32, math.log(20.0), math.log(80.0))), 20.0, 80.0),
        "parity": jax.random.randint(seeds[5], (1,), 0, 1073741824).astype(jnp.int32),
        "thresholds": plant(jax.random.randint(seeds[6], (WINDOWS,), 0, 1073741824), jax.random.fold_in(seeds[6], 1), 0, 1073741823).astype(jnp.int32),
    }


tiles_per_step = 16

def pair_energy(row_data, col_data, same_block, lambda_set):
    delta_x = row_data[0][:, :, None] - col_data[0][:, None, :]
    delta_y = row_data[1][:, :, None] - col_data[1][:, None, :]
    delta_z = row_data[2][:, :, None] - col_data[2][:, None, :]
    distance = delta_x * delta_x + delta_y * delta_y + delta_z * delta_z
    charge_pair = row_data[3][:, :, None] * col_data[3][:, None, :]
    well_depth = 4.0 * row_data[4][:, :, None] * col_data[4][:, None, :]
    size_pair = row_data[5][:, :, None] * col_data[5][:, None, :]
    scaled = distance / size_pair
    scaled_cube = scaled * scaled * scaled
    width_tile = distance.shape[-1]
    diagonal = (lax.broadcasted_iota(jnp.int32, (width_tile, width_tile), 0) == lax.broadcasted_iota(jnp.int32, (width_tile, width_tile), 1)).astype(jnp.float32)
    keep_mask = 1.0 - same_block[:, None, None] * diagonal[None]
    totals = []
    for number in range(3):
        lam_now = lambda_set[number]
        softened = 1.0 - 0.5 * lam_now + scaled_cube
        inverse = 1.0 / softened
        dispersion = well_depth * (inverse * inverse - inverse)
        coulomb = charge_pair * lax.rsqrt(distance + 2.0 - lam_now)
        totals.append(lam_now * jnp.sum(keep_mask * (dispersion + coulomb)))
    return jnp.stack(totals)

def window_sums(table, row_ids, col_ids, lambda_set):
    blocks = table.reshape(table.shape[0], -1, TILE)
    row_all = jnp.take(blocks, row_ids, axis=1)
    col_all = jnp.take(blocks, col_ids, axis=1)
    same_all = (row_ids == col_ids).astype(jnp.float32)
    count = row_ids.shape[0] // tiles_per_step

    def advance(number, total):
        start = number * tiles_per_step
        row_part = lax.dynamic_slice_in_dim(row_all, start, tiles_per_step, 1)
        col_part = lax.dynamic_slice_in_dim(col_all, start, tiles_per_step, 1)
        same_part = lax.dynamic_slice_in_dim(same_all, start, tiles_per_step, 0)
        return total + pair_energy(row_part, col_part, same_part, lambda_set)
    return lax.fori_loop(0, count, advance, jnp.zeros((3,), jnp.float32))

def reference(atom_table, row_blocks, col_blocks, lambdas, inverse_temp, parity, thresholds):
    windows = lambdas.shape[0]
    window = jnp.arange(windows, dtype=jnp.int32)
    below = jnp.clip(window - 1, 0, windows - 1)
    above = jnp.clip(window + 1, 0, windows - 1)
    lambda_sets = jnp.stack([lambdas[below], lambdas, lambdas[above]], axis=1)
    sums = lax.map(lambda pack: window_sums(pack[0], pack[1], pack[2], pack[3]), (atom_table, row_blocks, col_blocks, lambda_sets))
    energies = sums / (row_blocks.shape[1] * TILE * TILE)
    d_plus = energies[:, 2] - energies[:, 1]
    d_minus = energies[:, 0] - energies[:, 1]
    profile = jnp.concatenate([jnp.zeros((1,), jnp.float32), jnp.cumsum(d_plus)[:-1]])
    lower_win = jnp.where(jnp.remainder(window - parity[0], 2) == 0, window, window - 1)
    upper_win = lower_win + 1
    has_partner = (lower_win >= 0) & (upper_win < windows)
    lower_safe = jnp.clip(lower_win, 0, windows - 1)
    upper_safe = jnp.clip(upper_win, 0, windows - 1)
    change = d_plus[lower_safe] + d_minus[upper_safe]
    offset_draw = jnp.remainder(thresholds[lower_safe] + parity[0], 1073741824).astype(jnp.int32) + 1
    draw_share = offset_draw.astype(jnp.float32) / 1073741824.0
    margins = jnp.where(has_partner, -jnp.log(draw_share) - inverse_temp[0] * change, 0.0)
    return (energies, margins, profile)
```

```python
import functools

import jax
import jax.numpy as jnp
from jax import lax
from jax.experimental import pallas as pl
from jax.experimental.pallas import tpu as pltpu
from jax.sharding import PartitionSpec as P

TILE = 128
SUB = 8
FIELDS = 6
LINE = 4
SLOTS = 2
MESH = pl.DeviceIdType.MESH


def kernel(
    sizes,
    table_hbm,
    rows_hbm,
    cols_hbm,
    lam_hbm,
    beta_hbm,
    parity_hbm,
    thresh_hbm,
    energy_ref,
    margin_ref,
    profile_ref,
    table,
    rows,
    cols_s,
    cols,
    lam,
    beta,
    parity,
    thresh,
    line_inner,
    line_edge,
    rot,
    req,
    asked,
    pos,
    where_s,
    send_inner,
    send_edge,
    col_inner,
    col_edge,
    part,
    parts,
    local_sem,
    line_send,
    line_recv,
    req_send,
    req_recv,
    rep_send,
    rep_recv,
    sum_send,
    sum_recv,
):
    wins, groups, own, listed = sizes
    lines = groups // LINE
    per_line = LINE * SLOTS
    win = lax.axis_index("win")
    me = lax.axis_index("grp")
    my_line = me // LINE
    my_x = lax.rem(me, LINE)
    inner = 1 - win
    edge = win
    line_buf = (line_inner, line_edge)
    send_buf = (send_inner, send_edge)
    col_buf = (col_inner, col_edge)

    barrier = pltpu.get_barrier_semaphore()

    for step in range(1, lines):
        pl.semaphore_signal(barrier, inc=1, device_id=(win, lax.rem(my_line + step, lines) * LINE + my_x), device_id_type=MESH)
    for step in range(1, LINE):
        pl.semaphore_signal(barrier, inc=1, device_id=(win, my_line * LINE + lax.rem(my_x + step, LINE)), device_id_type=MESH)
    pl.semaphore_signal(barrier, inc=1, device_id=(1 - win, me), device_id_type=MESH)

    local = [
        pltpu.make_async_copy(src, dst, local_sem.at[number])
        for number, (src, dst) in enumerate(
            [
                (cols_hbm, cols),
                (table_hbm, table),
                (rows_hbm, rows),
                (cols_hbm, cols_s),
                (lam_hbm, lam),
                (beta_hbm, beta),
                (parity_hbm, parity),
                (thresh_hbm, thresh),
            ]
        )
    ]
    for copy in local:
        copy.start()

    local[0].wait()
    col_pair = cols[...]
    iota_line = lax.broadcasted_iota(jnp.int32, (lines, listed), 0)
    before = (
        lax.broadcasted_iota(jnp.int32, (listed, listed), 0)
        < lax.broadcasted_iota(jnp.int32, (listed, listed), 1)
    ).astype(jnp.float32)
    slot_iota = lax.broadcasted_iota(jnp.int32, (lines * per_line, listed), 0)
    for order, number in enumerate((inner, edge)):
        ids = jnp.where(number == 0, col_pair[0:1], col_pair[1:2])
        line_ids = jnp.zeros_like(ids)
        for bound in range(1, lines):
            line_ids += (ids >= bound * LINE * own).astype(jnp.int32)
        within = (ids - line_ids * (LINE * own)).astype(jnp.float32)
        hot = (line_ids == iota_line).astype(jnp.float32)
        earlier = jnp.dot(hot, before, preferred_element_type=jnp.float32)
        rank = jnp.sum(hot * earlier, axis=0, keepdims=True).astype(jnp.int32)
        place = line_ids * per_line + rank
        chosen = (place == slot_iota).astype(jnp.float32)
        asks = lax.dot_general(
            within, chosen, (((1,), (1,)), ((), ())), preferred_element_type=jnp.float32
        )
        req[order : order + 1, :] = asks.astype(jnp.int32)
        pos[order : order + 1, :listed] = place
    to_scalar = pltpu.make_async_copy(pos, where_s, local_sem.at[8])
    to_scalar.start()

    local[1].wait()
    for order, number in enumerate((inner, edge)):
        for field in range(FIELDS):
            pair = table[field]
            row = jnp.where(number == 0, pair[0:1], pair[1:2])
            if field == 5:
                row = 1.0 / row
            for block in range(own):
                line_buf[order][my_x * own + block, field : field + 1, :] = row[
                    :, block * TILE : (block + 1) * TILE
                ]

    pl.semaphore_wait(barrier, lines + LINE - 1)

    def plane(step):
        return lax.rem(my_line + step, lines)

    def request(step):
        return pltpu.make_async_remote_copy(
            src_ref=req,
            dst_ref=asked.at[my_line],
            send_sem=req_send,
            recv_sem=req_recv,
            device_id=(win, plane(step) * LINE + my_x),
            device_id_type=MESH,
        )

    for step in range(1, lines):
        request(step).start()
    own_request = pltpu.make_async_copy(req, asked.at[my_line], local_sem.at[9])
    own_request.start()

    def share(order, step):
        return pltpu.make_async_remote_copy(
            src_ref=line_buf[order].at[pl.ds(my_x * own, own)],
            dst_ref=line_buf[order].at[pl.ds(my_x * own, own)],
            send_sem=line_send.at[order],
            recv_sem=line_recv.at[order],
            device_id=(win, my_line * LINE + lax.rem(my_x + step, LINE)),
            device_id_type=MESH,
        )

    for order in range(2):
        for step in (2, 1, 3):
            share(order, step).start()

    def rotate(number, carry):
        for order in range(2):
            block = line_buf[order][my_x * own + number]
            for field in range(FIELDS):
                row = jnp.broadcast_to(block[field : field + 1], (SUB, TILE))
                if field == 4:
                    row = 4.0 * row
                for tile in range(TILE // SUB):
                    rot[order, number, field, tile * SUB : (tile + 1) * SUB, :] = pltpu.roll(
                        row, tile * SUB, 1, stride=1, stride_axis=0
                    )
        return carry

    lax.fori_loop(0, own, rotate, 0)

    for copy in local[2:]:
        copy.wait()
    to_scalar.wait()

    own_request.wait()
    pltpu.make_async_copy(
        asked.at[pl.ds(0, lines - 1)], asked.at[pl.ds(0, lines - 1)], req_recv
    ).wait()

    def reply(order, step):
        return pltpu.make_async_remote_copy(
            src_ref=send_buf[order].at[step - 1],
            dst_ref=col_buf[order].at[pl.ds(my_line * per_line, per_line)],
            send_sem=rep_send.at[order],
            recv_sem=rep_recv.at[order],
            device_id=(win, plane(step) * LINE + my_x),
            device_id_type=MESH,
        )

    for order in range(2):
        pltpu.make_async_copy(
            line_buf[order].at[pl.ds(0, own * (LINE - 1))],
            line_buf[order].at[pl.ds(0, own * (LINE - 1))],
            line_recv.at[order],
        ).wait()

        def serve(step, carry, order=order):
            peer = plane(step)
            for slot in range(per_line):
                wanted = jnp.clip(asked[peer, order, my_line * per_line + slot], 0, LINE * own - 1)
                send_buf[order][step - 1, slot] = line_buf[order][wanted]
            reply(order, step).start()
            return carry

        lax.fori_loop(1, lines, serve, 0)
        for slot in range(per_line):
            wanted = jnp.clip(asked[my_line, order, my_line * per_line + slot], 0, LINE * own - 1)
            col_buf[order][my_line * per_line + slot] = line_buf[order][wanted]

    first_sub = lax.broadcasted_iota(jnp.int32, (SUB, TILE), 0) == 0
    lane = lax.broadcasted_iota(jnp.int32, (1, TILE), 1)
    out_row = jnp.zeros((1, TILE), jnp.float32)
    count = 0
    for order, number in enumerate((inner, edge)):
        pltpu.make_async_copy(
            col_buf[order].at[pl.ds(0, (lines - 1) * per_line)],
            col_buf[order].at[pl.ds(0, (lines - 1) * per_line)],
            rep_recv.at[order],
        ).wait()
        if order == 0:
            lams = [lam[win + k] for k in range(3)]
        else:
            lams = [lam[2 * win + k] for k in range(2)]
        base = [jnp.full((SUB, TILE), 1.0 - 0.5 * l, jnp.float32) for l in lams]
        soft = [jnp.full((SUB, TILE), 2.0 - l, jnp.float32) for l in lams]

        def pair(p, totals, order=order, number=number, base=base, soft=soft):
            row_id = rows[number, p]
            local_row = jnp.clip(row_id - me * own, 0, own - 1)
            same = row_id == cols_s[number, p]
            drop = jnp.where(same, 0.0, 1.0)
            keep = jnp.where(first_sub, drop, 1.0)
            place = jnp.clip(where_s[order, p], 0, lines * per_line - 1)
            tile = col_buf[order][place]
            xj, yj, zj, qj, ej, sj = [
                jnp.broadcast_to(tile[f : f + 1], (SUB, TILE)) for f in range(FIELDS)
            ]
            disp = [jnp.zeros((SUB, TILE), jnp.float32) for _ in base]
            coul = [jnp.zeros((SUB, TILE), jnp.float32) for _ in base]
            for t in range(TILE // SUB):
                span = slice(t * SUB, (t + 1) * SUB)
                dx = rot[order, local_row, 0, span, :] - xj
                dy = rot[order, local_row, 1, span, :] - yj
                dz = rot[order, local_row, 2, span, :] - zj
                qi = rot[order, local_row, 3, span, :]
                ei = rot[order, local_row, 4, span, :]
                si = rot[order, local_row, 5, span, :]
                if t == 0:
                    qi = qi * keep
                    ei = ei * keep
                r2 = dx * dx + dy * dy + dz * dz
                u = r2 * si * sj
                v = u * u * u
                for k in range(len(base)):
                    inv = 1.0 / (base[k] + v)
                    disp[k] += ei * (inv * inv - inv)
                    coul[k] += qi * lax.rsqrt(r2 + soft[k])
            return tuple(
                total + ej * d + qj * c for total, d, c in zip(totals, disp, coul)
            )

        zero = jnp.zeros((SUB, TILE), jnp.float32)
        totals = lax.fori_loop(0, listed, pair, tuple(zero for _ in lams))
        for total, l in zip(totals, lams):
            out_row = jnp.where(lane == count, jnp.sum(total, keepdims=True) * l, out_row)
            count += 1

    flat = win * groups + me
    part[...] = out_row
    parts[flat] = out_row

    def tell(target_win, target):
        return pltpu.make_async_remote_copy(
            src_ref=part,
            dst_ref=parts.at[flat],
            send_sem=sum_send,
            recv_sem=sum_recv,
            device_id=(target_win, target),
            device_id_type=MESH,
        )

    def tell_all(step, carry):
        other = lax.rem(me + step, groups)
        tell(win, other).start()
        tell(1 - win, other).start()
        return carry

    lax.fori_loop(1, groups, tell_all, 0)
    tell(1 - win, me).start()

    pltpu.make_async_copy(asked.at[pl.ds(0, lines - 1)], asked.at[pl.ds(0, lines - 1)], req_send).wait()
    for order in range(2):
        pltpu.make_async_copy(
            line_buf[order].at[pl.ds(0, own * (LINE - 1))],
            line_buf[order].at[pl.ds(0, own * (LINE - 1))],
            line_send.at[order],
        ).wait()
        pltpu.make_async_copy(send_buf[order], send_buf[order], rep_send.at[order]).wait()

    par = parity[0]
    windows = 4
    firsts = [wins * win, wins * win + 1]
    even = lax.rem(par, 2) == 0

    everyone = pltpu.make_async_copy(
        parts.at[pl.ds(0, wins * groups - 1)], parts.at[pl.ds(0, wins * groups - 1)], sum_recv
    )
    lows = []
    logs = []
    for w in firsts:
        same_par = lax.rem(w, 2) == lax.rem(par, 2)
        low = jnp.where(same_par, w, w - 1)
        has = (low >= 0) & (low + 1 < windows)
        safe = jnp.clip(low, 0, windows - 1)
        draw = ((thresh[safe] + par) & 1073741823) + 1
        share_of = jnp.full((SUB, TILE), draw, jnp.int32).astype(jnp.float32) / 1073741824.0
        logs.append(-jnp.log(share_of)[0, 0])
        lows.append((low, has))
    everyone.wait()
    pltpu.make_async_copy(
        parts.at[pl.ds(0, wins * groups - 1)], parts.at[pl.ds(0, wins * groups - 1)], sum_send
    ).wait()

    def total_of(start):
        chains = [parts[start + k] for k in range(8)]
        for n in range(8, groups):
            chains[n % 8] = chains[n % 8] + parts[start + n]
        while len(chains) > 1:
            chains = [chains[2 * n] + chains[2 * n + 1] for n in range(len(chains) // 2)]
        return chains[0] * (1.0 / (listed * groups * TILE * TILE))

    first, second = total_of(0), total_of(groups)
    a = [first[0, k] for k in range(5)]
    b = [second[0, k] for k in range(5)]
    energies = [
        (a[3], a[3], a[4]),
        (a[0], a[1], a[2]),
        (b[0], b[1], b[2]),
        (b[3], b[4], b[4]),
    ]
    up = [e[2] - e[1] for e in energies]
    down = [e[0] - e[1] for e in energies]
    prof = [0.0, up[0], up[0] + up[1], up[0] + up[1] + up[2]]
    changes = [up[n] + down[n + 1] for n in range(3)]
    for n in range(2):
        for k in range(3):
            energy_ref[n, k] = jnp.where(win == 0, energies[n][k], energies[2 + n][k])
        profile_ref[n] = jnp.where(win == 0, prof[n], prof[2 + n])
        low, has = lows[n]
        change = jnp.where(low <= 0, changes[0], jnp.where(low == 1, changes[1], changes[2]))
        margin_ref[n] = jnp.where(has, logs[n] - beta[0] * change, 0.0)


def per_device(atom_table, row_blocks, col_blocks, lambdas, inverse_temp, parity, thresholds):
    wins = lax.axis_size("win")
    groups = lax.axis_size("grp")
    own = atom_table.shape[2] // TILE
    listed = row_blocks.shape[1]
    lines = groups // LINE
    per_line = LINE * SLOTS
    hbm = pl.BlockSpec(memory_space=pl.ANY)
    smem = pl.BlockSpec(memory_space=pltpu.SMEM)
    f32, i32 = jnp.float32, jnp.int32
    return pl.pallas_call(
        functools.partial(kernel, (wins, groups, own, listed)),
        out_shape=(
            jax.ShapeDtypeStruct((2, 3), f32),
            jax.ShapeDtypeStruct((2,), f32),
            jax.ShapeDtypeStruct((2,), f32),
        ),
        in_specs=[hbm] * 7,
        out_specs=(smem, smem, smem),
        scratch_shapes=[
            pltpu.VMEM((FIELDS, 2, own * TILE), f32),
            pltpu.SMEM((2, listed), i32),
            pltpu.SMEM((2, listed), i32),
            pltpu.VMEM((2, listed), i32),
            pltpu.SMEM((4,), f32),
            pltpu.SMEM((1,), f32),
            pltpu.SMEM((1,), i32),
            pltpu.SMEM((4,), i32),
            pltpu.VMEM((LINE * own, FIELDS, TILE), f32),
            pltpu.VMEM((LINE * own, FIELDS, TILE), f32),
            pltpu.VMEM((2, own, FIELDS, TILE, TILE), f32),
            pltpu.VMEM((2, TILE), i32),
            pltpu.SMEM((lines, 2, TILE), i32),
            pltpu.VMEM((2, TILE), i32),
            pltpu.SMEM((2, TILE), i32),
            pltpu.VMEM((lines - 1, per_line, FIELDS, TILE), f32),
            pltpu.VMEM((lines - 1, per_line, FIELDS, TILE), f32),
            pltpu.VMEM((lines * per_line, FIELDS, TILE), f32),
            pltpu.VMEM((lines * per_line, FIELDS, TILE), f32),
            pltpu.VMEM((1, TILE), f32),
            pltpu.VMEM((wins * groups, 1, TILE), f32),
            pltpu.SemaphoreType.DMA((10,)),
            pltpu.SemaphoreType.DMA((2,)),
            pltpu.SemaphoreType.DMA((2,)),
            pltpu.SemaphoreType.DMA,
            pltpu.SemaphoreType.DMA,
            pltpu.SemaphoreType.DMA((2,)),
            pltpu.SemaphoreType.DMA((2,)),
            pltpu.SemaphoreType.DMA,
            pltpu.SemaphoreType.DMA,
        ],
        compiler_params=pltpu.CompilerParams(collective_id=0, has_side_effects=True),
        name="exchange",
    )(
        jnp.transpose(atom_table, (1, 0, 2)),
        row_blocks,
        col_blocks,
        lambdas,
        inverse_temp,
        parity,
        thresholds,
    )


def solution(mesh):
    return jax.shard_map(
        per_device,
        mesh=mesh,
        in_specs=(P("win", None, "grp"), P("win", "grp"), P("win", "grp"), P(), P(), P(), P()),
        out_specs=(P("win", None), P("win"), P("win")),
        check_vma=False,
    )
```

```python
import functools

import jax
import jax.numpy as jnp
from jax import lax
from jax.experimental import pallas as pl
from jax.experimental.pallas import tpu as pltpu
from jax.sharding import PartitionSpec as P

TILE = 128
SUB = 8
FIELDS = 6
LINE = 4
SLOTS = 2
MESH = pl.DeviceIdType.MESH


def hops(offset):
    return min(offset, LINE - offset)


def kernel(
    sizes,
    table_hbm,
    rows_hbm,
    cols_hbm,
    lam_hbm,
    beta_hbm,
    parity_hbm,
    thresh_hbm,
    energy_ref,
    margin_ref,
    profile_ref,
    table,
    rows,
    cols_s,
    cols,
    lam,
    beta,
    parity,
    thresh,
    line_inner,
    line_edge,
    rot,
    req,
    asked,
    pos,
    where_s,
    send_inner,
    send_edge,
    col_inner,
    col_edge,
    part,
    parts,
    local_sem,
    line_send,
    line_recv,
    req_send,
    req_recv,
    rep_send,
    rep_recv,
    sum_send,
    sum_recv,
):
    wins, groups, own, listed = sizes
    lines = groups // LINE
    per_line = LINE * SLOTS
    win = lax.axis_index("win")
    me = lax.axis_index("grp")
    my_line = me // LINE
    my_x = lax.rem(me, LINE)
    my_y = lax.rem(my_line, LINE)
    my_z = my_line // LINE
    near = sorted(range(1, lines), key=lambda s: hops(s // LINE) + hops(s % LINE))
    inner = 1 - win
    edge = win
    line_buf = (line_inner, line_edge)
    send_buf = (send_inner, send_edge)
    col_buf = (col_inner, col_edge)

    def plane(step):
        return lax.rem(my_z + step // LINE, LINE) * LINE + lax.rem(my_y + step % LINE, LINE)

    barrier = pltpu.get_barrier_semaphore()

    for step in reversed(near):
        pl.semaphore_signal(
            barrier, inc=1, device_id=(win, plane(step) * LINE + my_x), device_id_type=MESH
        )
    for step in range(1, LINE):
        pl.semaphore_signal(
            barrier,
            inc=1,
            device_id=(win, my_line * LINE + lax.rem(my_x + step, LINE)),
            device_id_type=MESH,
        )
    pl.semaphore_signal(barrier, inc=1, device_id=(1 - win, me), device_id_type=MESH)

    local = [
        pltpu.make_async_copy(src, dst, local_sem.at[number])
        for number, (src, dst) in enumerate(
            [
                (cols_hbm, cols),
                (table_hbm, table),
                (rows_hbm, rows),
                (cols_hbm, cols_s),
                (lam_hbm, lam),
                (beta_hbm, beta),
                (parity_hbm, parity),
                (thresh_hbm, thresh),
            ]
        )
    ]
    for copy in local:
        copy.start()

    local[0].wait()
    col_pair = cols[...]
    iota_line = lax.broadcasted_iota(jnp.int32, (lines, listed), 0)
    before = (
        lax.broadcasted_iota(jnp.int32, (listed, listed), 0)
        < lax.broadcasted_iota(jnp.int32, (listed, listed), 1)
    ).astype(jnp.float32)
    slot_iota = lax.broadcasted_iota(jnp.int32, (lines * per_line, listed), 0)
    for order, number in enumerate((inner, edge)):
        ids = jnp.where(number == 0, col_pair[0:1], col_pair[1:2])
        line_ids = jnp.zeros_like(ids)
        for bound in range(1, lines):
            line_ids += (ids >= bound * LINE * own).astype(jnp.int32)
        within = (ids - line_ids * (LINE * own)).astype(jnp.float32)
        hot = (line_ids == iota_line).astype(jnp.float32)
        earlier = jnp.dot(hot, before, preferred_element_type=jnp.float32)
        rank = jnp.sum(hot * earlier, axis=0, keepdims=True).astype(jnp.int32)
        place = line_ids * per_line + rank
        chosen = (place == slot_iota).astype(jnp.float32)
        asks = lax.dot_general(
            within, chosen, (((1,), (1,)), ((), ())), preferred_element_type=jnp.float32
        )
        req[order : order + 1, :] = asks.astype(jnp.int32)
        pos[order : order + 1, :listed] = place
    to_scalar = pltpu.make_async_copy(pos, where_s, local_sem.at[8])
    to_scalar.start()

    pl.semaphore_wait(barrier, lines + LINE - 1)

    def request(step):
        return pltpu.make_async_remote_copy(
            src_ref=req,
            dst_ref=asked.at[my_line],
            send_sem=req_send,
            recv_sem=req_recv.at[my_line],
            device_id=(win, plane(step) * LINE + my_x),
            device_id_type=MESH,
        )

    for step in reversed(near):
        request(step).start()
    own_request = pltpu.make_async_copy(req, asked.at[my_line], local_sem.at[9])
    own_request.start()

    local[1].wait()
    for order, number in enumerate((inner, edge)):
        for field in range(FIELDS):
            pair = table[field]
            row = jnp.where(number == 0, pair[0:1], pair[1:2])
            if field == 5:
                row = 1.0 / row
            for block in range(own):
                line_buf[order][my_x * own + block, field : field + 1, :] = row[
                    :, block * TILE : (block + 1) * TILE
                ]

    def share(order, step):
        return pltpu.make_async_remote_copy(
            src_ref=line_buf[order].at[pl.ds(my_x * own, own)],
            dst_ref=line_buf[order].at[pl.ds(my_x * own, own)],
            send_sem=line_send.at[order],
            recv_sem=line_recv.at[order],
            device_id=(win, my_line * LINE + lax.rem(my_x + step, LINE)),
            device_id_type=MESH,
        )

    for order in range(2):
        for step in (2, 1, 3):
            share(order, step).start()

    def rotate(number, carry):
        for order in range(2):
            block = line_buf[order][my_x * own + number]
            for field in range(FIELDS):
                row = jnp.broadcast_to(block[field : field + 1], (SUB, TILE))
                if field == 4:
                    row = 4.0 * row
                for tile in range(TILE // SUB):
                    rot[order, number, field, tile * SUB : (tile + 1) * SUB, :] = pltpu.roll(
                        row, tile * SUB, 1, stride=1, stride_axis=0
                    )
        return carry

    lax.fori_loop(0, own, rotate, 0)

    for copy in local[2:]:
        copy.wait()
    to_scalar.wait()

    own_request.wait()

    def reply(order, step):
        return pltpu.make_async_remote_copy(
            src_ref=send_buf[order].at[step - 1],
            dst_ref=col_buf[order].at[pl.ds(my_line * per_line, per_line)],
            send_sem=rep_send.at[order],
            recv_sem=rep_recv.at[order],
            device_id=(win, plane(step) * LINE + my_x),
            device_id_type=MESH,
        )

    for step in near:
        pltpu.make_async_copy(asked.at[0], asked.at[0], req_recv.at[plane(step)]).wait()
    for order in range(2):
        pltpu.make_async_copy(
            line_buf[order].at[pl.ds(0, own * (LINE - 1))],
            line_buf[order].at[pl.ds(0, own * (LINE - 1))],
            line_recv.at[order],
        ).wait()

        for step in reversed(near):
            peer = plane(step)
            for slot in range(per_line):
                wanted = jnp.clip(asked[peer, order, my_line * per_line + slot], 0, LINE * own - 1)
                send_buf[order][step - 1, slot] = line_buf[order][wanted]
            if order == 0:
                reply(order, step).start()
        for slot in range(per_line):
            wanted = jnp.clip(asked[my_line, order, my_line * per_line + slot], 0, LINE * own - 1)
            col_buf[order][my_line * per_line + slot] = line_buf[order][wanted]

    first_sub = lax.broadcasted_iota(jnp.int32, (SUB, TILE), 0) == 0
    lane = lax.broadcasted_iota(jnp.int32, (1, TILE), 1)
    out_row = jnp.zeros((1, TILE), jnp.float32)
    count = 0
    for order, number in enumerate((inner, edge)):
        pltpu.make_async_copy(
            col_buf[order].at[pl.ds(0, (lines - 1) * per_line)],
            col_buf[order].at[pl.ds(0, (lines - 1) * per_line)],
            rep_recv.at[order],
        ).wait()
        if order == 0:

            for step in reversed(near):
                reply(1, step).start()
            lams = [lam[win + k] for k in range(3)]
        else:
            lams = [lam[2 * win + k] for k in range(2)]
        base = [jnp.full((SUB, TILE), 1.0 - 0.5 * l, jnp.float32) for l in lams]
        soft = [jnp.full((SUB, TILE), 2.0 - l, jnp.float32) for l in lams]

        def pair(p, totals, order=order, number=number, base=base, soft=soft):
            row_id = rows[number, p]
            local_row = jnp.clip(row_id - me * own, 0, own - 1)
            same = row_id == cols_s[number, p]
            drop = jnp.where(same, 0.0, 1.0)
            keep = jnp.where(first_sub, drop, 1.0)
            place = jnp.clip(where_s[order, p], 0, lines * per_line - 1)
            tile = col_buf[order][place]
            xj, yj, zj, qj, ej, sj = [
                jnp.broadcast_to(tile[f : f + 1], (SUB, TILE)) for f in range(FIELDS)
            ]
            disp = [jnp.zeros((SUB, TILE), jnp.float32) for _ in base]
            coul = [jnp.zeros((SUB, TILE), jnp.float32) for _ in base]
            for t in range(TILE // SUB):
                span = slice(t * SUB, (t + 1) * SUB)
                dx = rot[order, local_row, 0, span, :] - xj
                dy = rot[order, local_row, 1, span, :] - yj
                dz = rot[order, local_row, 2, span, :] - zj
                qi = rot[order, local_row, 3, span, :]
                ei = rot[order, local_row, 4, span, :]
                si = rot[order, local_row, 5, span, :]
                if t == 0:
                    qi = qi * keep
                    ei = ei * keep
                r2 = dx * dx + dy * dy + dz * dz
                u = r2 * si * sj
                v = u * u * u
                for k in range(len(base)):
                    inv = 1.0 / (base[k] + v)
                    disp[k] += ei * (inv * inv - inv)
                    coul[k] += qi * lax.rsqrt(r2 + soft[k])
            return tuple(
                total + ej * d + qj * c for total, d, c in zip(totals, disp, coul)
            )

        zero = jnp.zeros((SUB, TILE), jnp.float32)
        totals = lax.fori_loop(0, listed, pair, tuple(zero for _ in lams), unroll=8)
        for total, l in zip(totals, lams):
            out_row = jnp.where(lane == count, jnp.sum(total, keepdims=True) * l, out_row)
            count += 1

    flat = win * groups + me
    part[...] = out_row
    parts[flat] = out_row

    def tell(target_win, target):
        return pltpu.make_async_remote_copy(
            src_ref=part,
            dst_ref=parts.at[flat],
            send_sem=sum_send,
            recv_sem=sum_recv,
            device_id=(target_win, target),
            device_id_type=MESH,
        )

    def away(step):
        return hops(step // (LINE * LINE)) + hops(step // LINE % LINE) + hops(step % LINE)

    for step in sorted(range(groups), key=away, reverse=True):
        other = plane(step // LINE) * LINE + lax.rem(my_x + step % LINE, LINE)
        tell(1 - win, other).start()
        if step:
            tell(win, other).start()

    pltpu.make_async_copy(asked.at[pl.ds(0, lines - 1)], asked.at[pl.ds(0, lines - 1)], req_send).wait()
    for order in range(2):
        pltpu.make_async_copy(
            line_buf[order].at[pl.ds(0, own * (LINE - 1))],
            line_buf[order].at[pl.ds(0, own * (LINE - 1))],
            line_send.at[order],
        ).wait()
        pltpu.make_async_copy(send_buf[order], send_buf[order], rep_send.at[order]).wait()

    par = parity[0]
    windows = 4
    firsts = [wins * win, wins * win + 1]
    even = lax.rem(par, 2) == 0

    everyone = pltpu.make_async_copy(
        parts.at[pl.ds(0, wins * groups - 1)], parts.at[pl.ds(0, wins * groups - 1)], sum_recv
    )
    lows = []
    logs = []
    for w in firsts:
        same_par = lax.rem(w, 2) == lax.rem(par, 2)
        low = jnp.where(same_par, w, w - 1)
        has = (low >= 0) & (low + 1 < windows)
        safe = jnp.clip(low, 0, windows - 1)
        draw = ((thresh[safe] + par) & 1073741823) + 1
        share_of = jnp.full((SUB, TILE), draw, jnp.int32).astype(jnp.float32) / 1073741824.0
        logs.append(-jnp.log(share_of)[0, 0])
        lows.append((low, has))
    everyone.wait()
    pltpu.make_async_copy(
        parts.at[pl.ds(0, wins * groups - 1)], parts.at[pl.ds(0, wins * groups - 1)], sum_send
    ).wait()

    def total_of(start):
        chains = [parts[start + k] for k in range(8)]
        for n in range(8, groups):
            chains[n % 8] = chains[n % 8] + parts[start + n]
        while len(chains) > 1:
            chains = [chains[2 * n] + chains[2 * n + 1] for n in range(len(chains) // 2)]
        return chains[0] * (1.0 / (listed * groups * TILE * TILE))

    first, second = total_of(0), total_of(groups)
    a = [first[0, k] for k in range(5)]
    b = [second[0, k] for k in range(5)]
    energies = [
        (a[3], a[3], a[4]),
        (a[0], a[1], a[2]),
        (b[0], b[1], b[2]),
        (b[3], b[4], b[4]),
    ]
    up = [e[2] - e[1] for e in energies]
    down = [e[0] - e[1] for e in energies]
    prof = [0.0, up[0], up[0] + up[1], up[0] + up[1] + up[2]]
    changes = [up[n] + down[n + 1] for n in range(3)]
    for n in range(2):
        for k in range(3):
            energy_ref[n, k] = jnp.where(win == 0, energies[n][k], energies[2 + n][k])
        profile_ref[n] = jnp.where(win == 0, prof[n], prof[2 + n])
        low, has = lows[n]
        change = jnp.where(low <= 0, changes[0], jnp.where(low == 1, changes[1], changes[2]))
        margin_ref[n] = jnp.where(has, logs[n] - beta[0] * change, 0.0)


def per_device(atom_table, row_blocks, col_blocks, lambdas, inverse_temp, parity, thresholds):
    wins = lax.axis_size("win")
    groups = lax.axis_size("grp")
    own = atom_table.shape[2] // TILE
    listed = row_blocks.shape[1]
    lines = groups // LINE
    per_line = LINE * SLOTS
    hbm = pl.BlockSpec(memory_space=pl.ANY)
    smem = pl.BlockSpec(memory_space=pltpu.SMEM)
    f32, i32 = jnp.float32, jnp.int32
    results = pl.pallas_call(
        functools.partial(kernel, (wins, groups, own, listed)),
        out_shape=(
            jax.ShapeDtypeStruct((2, 3), f32),
            jax.ShapeDtypeStruct((2,), f32),
            jax.ShapeDtypeStruct((2,), f32),
        ),
        in_specs=[hbm] * 7,
        out_specs=(smem, smem, smem),
        scratch_shapes=[
            pltpu.VMEM((FIELDS, 2, own * TILE), f32),
            pltpu.SMEM((2, listed), i32),
            pltpu.SMEM((2, listed), i32),
            pltpu.VMEM((2, listed), i32),
            pltpu.SMEM((4,), f32),
            pltpu.SMEM((1,), f32),
            pltpu.SMEM((1,), i32),
            pltpu.SMEM((4,), i32),
            pltpu.VMEM((LINE * own, FIELDS, TILE), f32),
            pltpu.VMEM((LINE * own, FIELDS, TILE), f32),
            pltpu.VMEM((2, own, FIELDS, TILE, TILE), f32),
            pltpu.VMEM((2, TILE), i32),
            pltpu.SMEM((lines, 2, TILE), i32),
            pltpu.VMEM((2, TILE), i32),
            pltpu.SMEM((2, TILE), i32),
            pltpu.VMEM((lines - 1, per_line, FIELDS, TILE), f32),
            pltpu.VMEM((lines - 1, per_line, FIELDS, TILE), f32),
            pltpu.VMEM((lines * per_line, FIELDS, TILE), f32),
            pltpu.VMEM((lines * per_line, FIELDS, TILE), f32),
            pltpu.VMEM((1, TILE), f32),
            pltpu.VMEM((wins * groups, 1, TILE), f32),
            pltpu.SemaphoreType.DMA((10,)),
            pltpu.SemaphoreType.DMA((2,)),
            pltpu.SemaphoreType.DMA((2,)),
            pltpu.SemaphoreType.DMA,
            pltpu.SemaphoreType.DMA((lines,)),
            pltpu.SemaphoreType.DMA((2,)),
            pltpu.SemaphoreType.DMA((2,)),
            pltpu.SemaphoreType.DMA,
            pltpu.SemaphoreType.DMA,
        ],
        compiler_params=pltpu.CompilerParams(collective_id=0, has_side_effects=True),
        name="exchange",
    )(
        jnp.transpose(atom_table, (1, 0, 2)),
        row_blocks,
        col_blocks,
        lambdas,
        inverse_temp,
        parity,
        thresholds,
    )

    def hand_over(*refs):
        copies = [pltpu.make_async_copy(refs[n], refs[3 + n], refs[6].at[n]) for n in range(3)]
        for copy in copies:
            copy.start()
        for copy in copies:
            copy.wait()

    return pl.pallas_call(
        hand_over,
        out_shape=tuple(jax.ShapeDtypeStruct(r.shape, r.dtype) for r in results),
        in_specs=[hbm] * 3,
        out_specs=(hbm,) * 3,
        scratch_shapes=[pltpu.SemaphoreType.DMA((3,))],
        name="hand_over",
    )(*results)


def solution(mesh):
    return jax.shard_map(
        per_device,
        mesh=mesh,
        in_specs=(P("win", None, "grp"), P("win", "grp"), P("win", "grp"), P(), P(), P(), P()),
        out_specs=(P("win", None), P("win"), P("win")),
        check_vma=False,
    )
```

```python
import functools

import jax
import jax.numpy as jnp
from jax import lax
from jax.experimental import pallas as pl
from jax.experimental.pallas import tpu as pltpu
from jax.sharding import PartitionSpec as P

TILE = 128
SUB = 8
FIELDS = 6
LINE = 4
SLOTS = 2
MESH = pl.DeviceIdType.MESH


def hops(offset):
    return min(offset, LINE - offset)


def kernel(
    sizes,
    table_hbm,
    rows_hbm,
    cols_hbm,
    lam_hbm,
    beta_hbm,
    parity_hbm,
    thresh_hbm,
    energy_ref,
    margin_ref,
    profile_ref,
    table,
    rows,
    cols_s,
    cols,
    lam,
    beta,
    parity,
    thresh,
    line_inner,
    line_edge,
    rot,
    req,
    asked,
    pos,
    where_s,
    send_inner,
    send_edge,
    col_inner,
    col_edge,
    part,
    parts,
    local_sem,
    line_send,
    line_recv,
    req_send,
    req_recv,
    rep_send,
    rep_recv,
    sum_send,
    sum_recv,
):
    wins, groups, own, listed = sizes
    lines = groups // LINE
    per_line = LINE * SLOTS
    win = lax.axis_index("win")
    me = lax.axis_index("grp")
    my_line = me // LINE
    my_x = lax.rem(me, LINE)
    my_y = lax.rem(my_line, LINE)
    my_z = my_line // LINE
    near = sorted(range(1, lines), key=lambda s: hops(s // LINE) + hops(s % LINE))
    inner = 1 - win
    edge = win
    line_buf = (line_inner, line_edge)
    send_buf = (send_inner, send_edge)
    col_buf = (col_inner, col_edge)

    def plane(step):
        return lax.rem(my_z + step // LINE, LINE) * LINE + lax.rem(my_y + step % LINE, LINE)

    barrier = pltpu.get_barrier_semaphore()

    local = [
        pltpu.make_async_copy(src, dst, local_sem.at[number])
        for number, (src, dst) in enumerate(
            [
                (cols_hbm, cols),
                (table_hbm, table),
                (rows_hbm, rows),
                (cols_hbm, cols_s),
                (lam_hbm, lam),
                (beta_hbm, beta),
                (parity_hbm, parity),
                (thresh_hbm, thresh),
            ]
        )
    ]
    for copy in local:
        copy.start()

    for step in reversed(near):
        pl.semaphore_signal(
            barrier, inc=1, device_id=(win, plane(step) * LINE + my_x), device_id_type=MESH
        )
    for step in range(1, LINE):
        pl.semaphore_signal(
            barrier,
            inc=1,
            device_id=(win, my_line * LINE + lax.rem(my_x + step, LINE)),
            device_id_type=MESH,
        )
    pl.semaphore_signal(barrier, inc=1, device_id=(1 - win, me), device_id_type=MESH)

    local[0].wait()
    col_pair = cols[...]
    iota_line = lax.broadcasted_iota(jnp.int32, (lines, listed), 0)
    before = (
        lax.broadcasted_iota(jnp.int32, (listed, listed), 0)
        < lax.broadcasted_iota(jnp.int32, (listed, listed), 1)
    ).astype(jnp.float32)
    slot_iota = lax.broadcasted_iota(jnp.int32, (lines * per_line, listed), 0)
    for order, number in enumerate((inner, edge)):
        ids = jnp.where(number == 0, col_pair[0:1], col_pair[1:2])
        line_ids = jnp.zeros_like(ids)
        for bound in range(1, lines):
            line_ids += (ids >= bound * LINE * own).astype(jnp.int32)
        within = (ids - line_ids * (LINE * own)).astype(jnp.float32)
        hot = (line_ids == iota_line).astype(jnp.float32)
        earlier = jnp.dot(hot, before, preferred_element_type=jnp.float32)
        rank = jnp.sum(hot * earlier, axis=0, keepdims=True).astype(jnp.int32)
        place = line_ids * per_line + rank
        chosen = (place == slot_iota).astype(jnp.float32)
        asks = lax.dot_general(
            within, chosen, (((1,), (1,)), ((), ())), preferred_element_type=jnp.float32
        )
        req[order : order + 1, :] = asks.astype(jnp.int32)
        pos[order : order + 1, :listed] = place
    to_scalar = pltpu.make_async_copy(pos, where_s, local_sem.at[8])
    to_scalar.start()

    local[1].wait()
    for order, number in enumerate((inner, edge)):
        for field in range(FIELDS):
            pair = table[field]
            row = jnp.where(number == 0, pair[0:1], pair[1:2])
            if field == 5:
                row = 1.0 / row
            for block in range(own):
                line_buf[order][my_x * own + block, field : field + 1, :] = row[
                    :, block * TILE : (block + 1) * TILE
                ]

    pl.semaphore_wait(barrier, lines + LINE - 1)

    def request(step):
        return pltpu.make_async_remote_copy(
            src_ref=req,
            dst_ref=asked.at[my_line],
            send_sem=req_send,
            recv_sem=req_recv.at[my_line],
            device_id=(win, plane(step) * LINE + my_x),
            device_id_type=MESH,
        )

    for step in reversed(near):
        request(step).start()
    own_request = pltpu.make_async_copy(req, asked.at[my_line], local_sem.at[9])
    own_request.start()

    def share(order, step):
        return pltpu.make_async_remote_copy(
            src_ref=line_buf[order].at[pl.ds(my_x * own, own)],
            dst_ref=line_buf[order].at[pl.ds(my_x * own, own)],
            send_sem=line_send.at[order],
            recv_sem=line_recv.at[order],
            device_id=(win, my_line * LINE + lax.rem(my_x + step, LINE)),
            device_id_type=MESH,
        )

    for order in range(2):
        for step in (2, 1, 3):
            share(order, step).start()

    for copy in local[2:]:
        copy.wait()

    lam_sets = [[lam[win + k] for k in range(3)], [lam[2 * win + k] for k in range(2)]]

    def rotate(order):
        def turn(number, carry):
            block = line_buf[order][my_x * own + number]
            root = 2.0 * jnp.sqrt(block[4:5])
            scale = 1.0 / root
            turned = [
                block[0:1],
                block[1:2],
                block[2:3],
                block[3:4],
                root,
                block[5:6] * block[5:6] * block[5:6] * scale,
                scale,
            ]
            for field, row in enumerate(turned):
                row = jnp.broadcast_to(row, (SUB, TILE))
                for tile in range(TILE // SUB):
                    span = slice(tile * SUB, (tile + 1) * SUB)
                    value = pltpu.roll(row, tile * SUB, 1, stride=1, stride_axis=0)
                    if field < FIELDS:
                        rot[order, number, field, span, :] = value
                    else:
                        for k, l in enumerate(lam_sets[order]):
                            rot[order, number, field + k, span, :] = value * (1.0 - 0.5 * l)
            return carry

        lax.fori_loop(0, own, turn, 0)


    to_scalar.wait()

    own_request.wait()

    def reply(order, step):
        return pltpu.make_async_remote_copy(
            src_ref=send_buf[order].at[step - 1],
            dst_ref=col_buf[order].at[pl.ds(my_line * per_line, per_line)],
            send_sem=rep_send.at[order],
            recv_sem=rep_recv.at[order],
            device_id=(win, plane(step) * LINE + my_x),
            device_id_type=MESH,
        )

    for step in near:
        pltpu.make_async_copy(asked.at[0], asked.at[0], req_recv.at[plane(step)]).wait()
    for order in range(2):
        pltpu.make_async_copy(
            line_buf[order].at[pl.ds(0, own * (LINE - 1))],
            line_buf[order].at[pl.ds(0, own * (LINE - 1))],
            line_recv.at[order],
        ).wait()

        for step in reversed(near):
            peer = plane(step)
            for slot in range(per_line):
                wanted = jnp.clip(asked[peer, order, my_line * per_line + slot], 0, LINE * own - 1)
                send_buf[order][step - 1, slot] = line_buf[order][wanted]
            if order == 0:
                reply(order, step).start()
        for slot in range(per_line):
            wanted = jnp.clip(asked[my_line, order, my_line * per_line + slot], 0, LINE * own - 1)
            col_buf[order][my_line * per_line + slot] = line_buf[order][wanted]
        if order == 0:
            rotate(0)
            rotate(1)

    first_sub = lax.broadcasted_iota(jnp.int32, (SUB, TILE), 0) == 0
    lane = lax.broadcasted_iota(jnp.int32, (1, TILE), 1)
    out_row = jnp.zeros((1, TILE), jnp.float32)
    count = 0
    for order, number in enumerate((inner, edge)):
        pltpu.make_async_copy(
            col_buf[order].at[pl.ds(0, (lines - 1) * per_line)],
            col_buf[order].at[pl.ds(0, (lines - 1) * per_line)],
            rep_recv.at[order],
        ).wait()
        if order == 0:

            for step in reversed(near):
                reply(1, step).start()
        lams = lam_sets[order]
        soft = [jnp.full((SUB, TILE), 2.0 - l, jnp.float32) for l in lams]

        def pair(p, totals, order=order, number=number, soft=soft):
            row_id = rows[number, p]
            local_row = jnp.clip(row_id - me * own, 0, own - 1)
            same = row_id == cols_s[number, p]
            drop = jnp.where(same, 0.0, 1.0)
            keep = jnp.where(first_sub, drop, 1.0)
            place = jnp.clip(where_s[order, p], 0, lines * per_line - 1)
            tile = col_buf[order][place]
            xj, yj, zj, qj, ej, sj = [
                jnp.broadcast_to(tile[f : f + 1], (SUB, TILE)) for f in range(FIELDS)
            ]
            disp = [jnp.zeros((SUB, TILE), jnp.float32) for _ in soft]
            coul = [jnp.zeros((SUB, TILE), jnp.float32) for _ in soft]
            for t in range(TILE // SUB):
                span = slice(t * SUB, (t + 1) * SUB)
                dx = rot[order, local_row, 0, span, :] - xj
                dy = rot[order, local_row, 1, span, :] - yj
                dz = rot[order, local_row, 2, span, :] - zj
                qi = rot[order, local_row, 3, span, :]
                gi = rot[order, local_row, 4, span, :]
                ai = rot[order, local_row, 5, span, :]
                r2 = dx * dx + dy * dy + dz * dz
                u = r2 * sj
                v = u * u * u * ai
                if t == 0:
                    qi = qi * keep
                for k in range(len(soft)):
                    w = 1.0 / (rot[order, local_row, FIELDS + k, span, :] + v)
                    g = w * (w - gi)
                    disp[k] += g * keep if t == 0 else g
                    coul[k] += qi * lax.rsqrt(r2 + soft[k])
            return tuple(
                total + ej * d + qj * c for total, d, c in zip(totals, disp, coul)
            )

        zero = jnp.zeros((SUB, TILE), jnp.float32)
        totals = lax.fori_loop(0, listed, pair, tuple(zero for _ in lams), unroll=8)
        for total, l in zip(totals, lams):
            out_row = jnp.where(lane == count, jnp.sum(total, keepdims=True) * l, out_row)
            count += 1

    flat = win * groups + me
    part[...] = out_row
    parts[flat] = out_row

    def tell(target_win, target):
        return pltpu.make_async_remote_copy(
            src_ref=part,
            dst_ref=parts.at[flat],
            send_sem=sum_send,
            recv_sem=sum_recv,
            device_id=(target_win, target),
            device_id_type=MESH,
        )

    def away(step):
        return hops(step // (LINE * LINE)) + hops(step // LINE % LINE) + hops(step % LINE)

    for step in sorted(range(groups), key=away, reverse=True):
        other = plane(step // LINE) * LINE + lax.rem(my_x + step % LINE, LINE)
        tell(1 - win, other).start()
        if step:
            tell(win, other).start()

    pltpu.make_async_copy(asked.at[pl.ds(0, lines - 1)], asked.at[pl.ds(0, lines - 1)], req_send).wait()
    for order in range(2):
        pltpu.make_async_copy(
            line_buf[order].at[pl.ds(0, own * (LINE - 1))],
            line_buf[order].at[pl.ds(0, own * (LINE - 1))],
            line_send.at[order],
        ).wait()
        pltpu.make_async_copy(send_buf[order], send_buf[order], rep_send.at[order]).wait()

    par = parity[0]
    windows = 4
    firsts = [wins * win, wins * win + 1]
    even = lax.rem(par, 2) == 0

    everyone = pltpu.make_async_copy(
        parts.at[pl.ds(0, wins * groups - 1)], parts.at[pl.ds(0, wins * groups - 1)], sum_recv
    )
    lows = []
    logs = []
    for w in firsts:
        same_par = lax.rem(w, 2) == lax.rem(par, 2)
        low = jnp.where(same_par, w, w - 1)
        has = (low >= 0) & (low + 1 < windows)
        safe = jnp.clip(low, 0, windows - 1)
        draw = ((thresh[safe] + par) & 1073741823) + 1
        share_of = jnp.full((SUB, TILE), draw, jnp.int32).astype(jnp.float32) / 1073741824.0
        logs.append(-jnp.log(share_of)[0, 0])
        lows.append((low, has))
    everyone.wait()
    pltpu.make_async_copy(
        parts.at[pl.ds(0, wins * groups - 1)], parts.at[pl.ds(0, wins * groups - 1)], sum_send
    ).wait()

    def total_of(start):
        chains = [parts[start + k] for k in range(8)]
        for n in range(8, groups):
            chains[n % 8] = chains[n % 8] + parts[start + n]
        while len(chains) > 1:
            chains = [chains[2 * n] + chains[2 * n + 1] for n in range(len(chains) // 2)]
        return chains[0] * (1.0 / (listed * groups * TILE * TILE))

    first, second = total_of(0), total_of(groups)
    a = [first[0, k] for k in range(5)]
    b = [second[0, k] for k in range(5)]
    energies = [
        (a[3], a[3], a[4]),
        (a[0], a[1], a[2]),
        (b[0], b[1], b[2]),
        (b[3], b[4], b[4]),
    ]
    up = [e[2] - e[1] for e in energies]
    down = [e[0] - e[1] for e in energies]
    prof = [0.0, up[0], up[0] + up[1], up[0] + up[1] + up[2]]
    changes = [up[n] + down[n + 1] for n in range(3)]
    for n in range(2):
        for k in range(3):
            energy_ref[n, k] = jnp.where(win == 0, energies[n][k], energies[2 + n][k])
        profile_ref[n] = jnp.where(win == 0, prof[n], prof[2 + n])
        low, has = lows[n]
        change = jnp.where(low <= 0, changes[0], jnp.where(low == 1, changes[1], changes[2]))
        margin_ref[n] = jnp.where(has, logs[n] - beta[0] * change, 0.0)


def per_device(atom_table, row_blocks, col_blocks, lambdas, inverse_temp, parity, thresholds):
    wins = lax.axis_size("win")
    groups = lax.axis_size("grp")
    own = atom_table.shape[2] // TILE
    listed = row_blocks.shape[1]
    lines = groups // LINE
    per_line = LINE * SLOTS
    hbm = pl.BlockSpec(memory_space=pl.ANY)
    smem = pl.BlockSpec(memory_space=pltpu.SMEM)
    f32, i32 = jnp.float32, jnp.int32
    results = pl.pallas_call(
        functools.partial(kernel, (wins, groups, own, listed)),
        out_shape=(
            jax.ShapeDtypeStruct((2, 3), f32),
            jax.ShapeDtypeStruct((2,), f32),
            jax.ShapeDtypeStruct((2,), f32),
        ),
        in_specs=[hbm] * 7,
        out_specs=(smem, smem, smem),
        scratch_shapes=[
            pltpu.VMEM((FIELDS, 2, own * TILE), f32),
            pltpu.SMEM((2, listed), i32),
            pltpu.SMEM((2, listed), i32),
            pltpu.VMEM((2, listed), i32),
            pltpu.SMEM((4,), f32),
            pltpu.SMEM((1,), f32),
            pltpu.SMEM((1,), i32),
            pltpu.SMEM((4,), i32),
            pltpu.VMEM((LINE * own, FIELDS, TILE), f32),
            pltpu.VMEM((LINE * own, FIELDS, TILE), f32),
            pltpu.VMEM((2, own, FIELDS + 3, TILE, TILE), f32),
            pltpu.VMEM((2, TILE), i32),
            pltpu.SMEM((lines, 2, TILE), i32),
            pltpu.VMEM((2, TILE), i32),
            pltpu.SMEM((2, TILE), i32),
            pltpu.VMEM((lines - 1, per_line, FIELDS, TILE), f32),
            pltpu.VMEM((lines - 1, per_line, FIELDS, TILE), f32),
            pltpu.VMEM((lines * per_line, FIELDS, TILE), f32),
            pltpu.VMEM((lines * per_line, FIELDS, TILE), f32),
            pltpu.VMEM((1, TILE), f32),
            pltpu.VMEM((wins * groups, 1, TILE), f32),
            pltpu.SemaphoreType.DMA((10,)),
            pltpu.SemaphoreType.DMA((2,)),
            pltpu.SemaphoreType.DMA((2,)),
            pltpu.SemaphoreType.DMA,
            pltpu.SemaphoreType.DMA((lines,)),
            pltpu.SemaphoreType.DMA((2,)),
            pltpu.SemaphoreType.DMA((2,)),
            pltpu.SemaphoreType.DMA,
            pltpu.SemaphoreType.DMA,
        ],
        compiler_params=pltpu.CompilerParams(collective_id=0, has_side_effects=True),
        name="exchange",
    )(
        jnp.transpose(atom_table, (1, 0, 2)),
        row_blocks,
        col_blocks,
        lambdas,
        inverse_temp,
        parity,
        thresholds,
    )

    def hand_over(*refs):
        copies = [pltpu.make_async_copy(refs[n], refs[3 + n], refs[6].at[n]) for n in range(3)]
        for copy in copies:
            copy.start()
        for copy in copies:
            copy.wait()

    return pl.pallas_call(
        hand_over,
        out_shape=tuple(jax.ShapeDtypeStruct(r.shape, r.dtype) for r in results),
        in_specs=[hbm] * 3,
        out_specs=(hbm,) * 3,
        scratch_shapes=[pltpu.SemaphoreType.DMA((3,))],
        name="hand_over",
    )(*results)


def solution(mesh):
    return jax.shard_map(
        per_device,
        mesh=mesh,
        in_specs=(P("win", None, "grp"), P("win", "grp"), P("win", "grp"), P(), P(), P(), P()),
        out_specs=(P("win", None), P("win"), P("win")),
        check_vma=False,
    )
```

```python
import functools

import jax
import jax.numpy as jnp
from jax import lax
from jax.experimental import pallas as pl
from jax.experimental.pallas import tpu as pltpu
from jax.sharding import PartitionSpec as P

TILE = 128
SUB = 8
FIELDS = 6
LINE = 4
SLOTS = 2
MESH = pl.DeviceIdType.MESH


def hops(offset):
    return min(offset, LINE - offset)


def kernel(
    sizes,
    table_hbm,
    rows_hbm,
    cols_hbm,
    lam_hbm,
    beta_hbm,
    parity_hbm,
    thresh_hbm,
    energy_ref,
    margin_ref,
    profile_ref,
    table,
    rows,
    cols_s,
    cols,
    lam,
    beta,
    parity,
    thresh,
    line_inner,
    line_edge,
    rot,
    req,
    asked,
    pos,
    where_s,
    send_inner,
    send_edge,
    col_inner,
    col_edge,
    part,
    parts,
    local_sem,
    line_send,
    line_recv,
    req_send,
    req_recv,
    rep_send,
    rep_recv,
    sum_send,
    sum_recv,
):
    wins, groups, own, listed = sizes
    lines = groups // LINE
    per_line = LINE * SLOTS
    win = lax.axis_index("win")
    me = lax.axis_index("grp")
    my_line = me // LINE
    my_x = lax.rem(me, LINE)
    my_y = lax.rem(my_line, LINE)
    my_z = my_line // LINE
    near = sorted(range(1, lines), key=lambda s: hops(s // LINE) + hops(s % LINE))
    inner = 1 - win
    edge = win
    line_buf = (line_inner, line_edge)
    send_buf = (send_inner, send_edge)
    col_buf = (col_inner, col_edge)

    def plane(step):
        return lax.rem(my_z + step // LINE, LINE) * LINE + lax.rem(my_y + step % LINE, LINE)

    barrier = pltpu.get_barrier_semaphore()

    local = [
        pltpu.make_async_copy(src, dst, local_sem.at[number])
        for number, (src, dst) in enumerate(
            [
                (cols_hbm, cols),
                (table_hbm, table),
                (rows_hbm, rows),
                (cols_hbm, cols_s),
                (lam_hbm, lam),
                (beta_hbm, beta),
                (parity_hbm, parity),
                (thresh_hbm, thresh),
            ]
        )
    ]
    for copy in local:
        copy.start()

    for step in reversed(near):
        pl.semaphore_signal(
            barrier, inc=1, device_id=(win, plane(step) * LINE + my_x), device_id_type=MESH
        )
    for step in range(1, LINE):
        pl.semaphore_signal(
            barrier,
            inc=1,
            device_id=(win, my_line * LINE + lax.rem(my_x + step, LINE)),
            device_id_type=MESH,
        )
    pl.semaphore_signal(barrier, inc=1, device_id=(1 - win, me), device_id_type=MESH)

    local[0].wait()
    col_pair = cols[...]
    iota_line = lax.broadcasted_iota(jnp.int32, (lines, listed), 0)
    before = (
        lax.broadcasted_iota(jnp.int32, (listed, listed), 0)
        < lax.broadcasted_iota(jnp.int32, (listed, listed), 1)
    ).astype(jnp.float32)
    slot_iota = lax.broadcasted_iota(jnp.int32, (TILE, listed), 0)
    asks = jnp.zeros((lines, TILE), jnp.float32)
    for order, number in enumerate((inner, edge)):
        ids = jnp.where(number == 0, col_pair[0:1], col_pair[1:2])
        line_ids = jnp.zeros_like(ids)
        for bound in range(1, lines):
            line_ids += (ids >= bound * LINE * own).astype(jnp.int32)
        within = (ids - line_ids * (LINE * own)).astype(jnp.float32)
        hot = (line_ids == iota_line).astype(jnp.float32)
        earlier = jnp.dot(hot, before, preferred_element_type=jnp.float32)
        rank = jnp.sum(hot * earlier, axis=0, keepdims=True).astype(jnp.int32)
        place = line_ids * per_line + rank
        ranked = (rank + order * per_line == slot_iota).astype(jnp.float32)
        asks += lax.dot_general(
            hot * within, ranked, (((1,), (1,)), ((), ())), preferred_element_type=jnp.float32
        )
        pos[order : order + 1, :listed] = place
    asks = asks.astype(jnp.int32)
    for line in range(lines):
        req[line] = asks[line : line + 1]
    to_scalar = pltpu.make_async_copy(pos, where_s, local_sem.at[8])
    to_scalar.start()

    local[1].wait()
    for order, number in enumerate((inner, edge)):
        for field in range(FIELDS):
            pair = table[field]
            row = jnp.where(number == 0, pair[0:1], pair[1:2])
            if field == 5:
                row = 1.0 / row
            for block in range(own):
                line_buf[order][my_x * own + block, field : field + 1, :] = row[
                    :, block * TILE : (block + 1) * TILE
                ]

    pl.semaphore_wait(barrier, lines + LINE - 1)

    def request(step):
        return pltpu.make_async_remote_copy(
            src_ref=req.at[plane(step)],
            dst_ref=asked.at[my_line],
            send_sem=req_send,
            recv_sem=req_recv.at[my_line],
            device_id=(win, plane(step) * LINE + my_x),
            device_id_type=MESH,
        )

    for step in reversed(near):
        request(step).start()
    own_request = pltpu.make_async_copy(req.at[my_line], asked.at[my_line], local_sem.at[9])
    own_request.start()

    def share(order, step):
        return pltpu.make_async_remote_copy(
            src_ref=line_buf[order].at[pl.ds(my_x * own, own)],
            dst_ref=line_buf[order].at[pl.ds(my_x * own, own)],
            send_sem=line_send.at[order],
            recv_sem=line_recv.at[order],
            device_id=(win, my_line * LINE + lax.rem(my_x + step, LINE)),
            device_id_type=MESH,
        )

    for order in range(2):
        for step in (2, 1, 3):
            share(order, step).start()

    for copy in local[2:]:
        copy.wait()

    lam_sets = [[lam[win + k] for k in range(3)], [lam[2 * win + k] for k in range(2)]]

    def rotate(order):
        def turn(number, carry):
            block = line_buf[order][my_x * own + number]
            root = 2.0 * jnp.sqrt(block[4:5])
            scale = 1.0 / root
            turned = [
                block[0:1],
                block[1:2],
                block[2:3],
                block[3:4],
                root,
                block[5:6] * block[5:6] * block[5:6] * scale,
                scale,
            ]
            for field, row in enumerate(turned):
                row = jnp.broadcast_to(row, (SUB, TILE))
                for tile in range(TILE // SUB):
                    span = slice(tile * SUB, (tile + 1) * SUB)
                    value = pltpu.roll(row, tile * SUB, 1, stride=1, stride_axis=0)
                    if field < FIELDS:
                        rot[order, number, field, span, :] = value
                    else:
                        for k, l in enumerate(lam_sets[order]):
                            rot[order, number, field + k, span, :] = value * (1.0 - 0.5 * l)
            return carry

        lax.fori_loop(0, own, turn, 0)


    to_scalar.wait()

    own_request.wait()

    def reply(order, step):
        return pltpu.make_async_remote_copy(
            src_ref=send_buf[order].at[step - 1],
            dst_ref=col_buf[order].at[pl.ds(my_line * per_line, per_line)],
            send_sem=rep_send.at[order],
            recv_sem=rep_recv.at[order],
            device_id=(win, plane(step) * LINE + my_x),
            device_id_type=MESH,
        )

    for step in near:
        pltpu.make_async_copy(asked.at[0], asked.at[0], req_recv.at[plane(step)]).wait()
    for order in range(2):
        pltpu.make_async_copy(
            line_buf[order].at[pl.ds(0, own * (LINE - 1))],
            line_buf[order].at[pl.ds(0, own * (LINE - 1))],
            line_recv.at[order],
        ).wait()

        for step in reversed(near):
            peer = plane(step)
            for slot in range(per_line):
                wanted = jnp.clip(asked[peer, 0, order * per_line + slot], 0, LINE * own - 1)
                send_buf[order][step - 1, slot] = line_buf[order][wanted]
            if order == 0:
                reply(order, step).start()
        for slot in range(per_line):
            wanted = jnp.clip(asked[my_line, 0, order * per_line + slot], 0, LINE * own - 1)
            col_buf[order][my_line * per_line + slot] = line_buf[order][wanted]
        if order == 0:
            rotate(0)
            rotate(1)

    first_sub = lax.broadcasted_iota(jnp.int32, (SUB, TILE), 0) == 0
    lane = lax.broadcasted_iota(jnp.int32, (1, TILE), 1)
    out_row = jnp.zeros((1, TILE), jnp.float32)
    count = 0
    for order, number in enumerate((inner, edge)):
        pltpu.make_async_copy(
            col_buf[order].at[pl.ds(0, (lines - 1) * per_line)],
            col_buf[order].at[pl.ds(0, (lines - 1) * per_line)],
            rep_recv.at[order],
        ).wait()
        if order == 0:

            for step in reversed(near):
                reply(1, step).start()
        lams = lam_sets[order]
        soft = [jnp.full((SUB, TILE), 2.0 - l, jnp.float32) for l in lams]

        def pair(p, totals, order=order, number=number, soft=soft):
            row_id = rows[number, p]
            local_row = jnp.clip(row_id - me * own, 0, own - 1)
            same = row_id == cols_s[number, p]
            drop = jnp.where(same, 0.0, 1.0)
            keep = jnp.where(first_sub, drop, 1.0)
            place = jnp.clip(where_s[order, p], 0, lines * per_line - 1)
            tile = col_buf[order][place]
            xj, yj, zj, qj, ej, sj = [
                jnp.broadcast_to(tile[f : f + 1], (SUB, TILE)) for f in range(FIELDS)
            ]
            disp = [jnp.zeros((SUB, TILE), jnp.float32) for _ in soft]
            coul = [jnp.zeros((SUB, TILE), jnp.float32) for _ in soft]
            for t in range(TILE // SUB):
                span = slice(t * SUB, (t + 1) * SUB)
                dx = rot[order, local_row, 0, span, :] - xj
                dy = rot[order, local_row, 1, span, :] - yj
                dz = rot[order, local_row, 2, span, :] - zj
                qi = rot[order, local_row, 3, span, :]
                gi = rot[order, local_row, 4, span, :]
                ai = rot[order, local_row, 5, span, :]
                r2 = dx * dx + dy * dy + dz * dz
                u = r2 * sj
                v = u * u * u * ai
                if t == 0:
                    qi = qi * keep
                for k in range(len(soft)):
                    w = 1.0 / (rot[order, local_row, FIELDS + k, span, :] + v)
                    g = w * (w - gi)
                    disp[k] += g * keep if t == 0 else g
                    coul[k] += qi * lax.rsqrt(r2 + soft[k])
            return tuple(
                total + ej * d + qj * c for total, d, c in zip(totals, disp, coul)
            )

        zero = jnp.zeros((SUB, TILE), jnp.float32)
        totals = lax.fori_loop(0, listed, pair, tuple(zero for _ in lams), unroll=8)
        for total, l in zip(totals, lams):
            out_row = jnp.where(lane == count, jnp.sum(total, keepdims=True) * l, out_row)
            count += 1

    flat = win * groups + me
    part[...] = out_row
    parts[flat] = out_row

    def tell(target_win, target):
        return pltpu.make_async_remote_copy(
            src_ref=part,
            dst_ref=parts.at[flat],
            send_sem=sum_send,
            recv_sem=sum_recv,
            device_id=(target_win, target),
            device_id_type=MESH,
        )

    def away(step):
        return hops(step // (LINE * LINE)) + hops(step // LINE % LINE) + hops(step % LINE)

    for step in sorted(range(groups), key=away, reverse=True):
        other = plane(step // LINE) * LINE + lax.rem(my_x + step % LINE, LINE)
        tell(1 - win, other).start()
        if step:
            tell(win, other).start()

    pltpu.make_async_copy(asked.at[pl.ds(0, lines - 1)], asked.at[pl.ds(0, lines - 1)], req_send).wait()
    for order in range(2):
        pltpu.make_async_copy(
            line_buf[order].at[pl.ds(0, own * (LINE - 1))],
            line_buf[order].at[pl.ds(0, own * (LINE - 1))],
            line_send.at[order],
        ).wait()
        pltpu.make_async_copy(send_buf[order], send_buf[order], rep_send.at[order]).wait()

    par = parity[0]
    windows = 4
    firsts = [wins * win, wins * win + 1]
    even = lax.rem(par, 2) == 0

    everyone = pltpu.make_async_copy(
        parts.at[pl.ds(0, wins * groups - 1)], parts.at[pl.ds(0, wins * groups - 1)], sum_recv
    )
    lows = []
    logs = []
    for w in firsts:
        same_par = lax.rem(w, 2) == lax.rem(par, 2)
        low = jnp.where(same_par, w, w - 1)
        has = (low >= 0) & (low + 1 < windows)
        safe = jnp.clip(low, 0, windows - 1)
        draw = ((thresh[safe] + par) & 1073741823) + 1
        share_of = jnp.full((SUB, TILE), draw, jnp.int32).astype(jnp.float32) / 1073741824.0
        logs.append(-jnp.log(share_of)[0, 0])
        lows.append((low, has))
    everyone.wait()

    def total_of(start):
        chains = [parts[start + k] for k in range(8)]
        for n in range(8, groups):
            chains[n % 8] = chains[n % 8] + parts[start + n]
        while len(chains) > 1:
            chains = [chains[2 * n] + chains[2 * n + 1] for n in range(len(chains) // 2)]
        return chains[0] * (1.0 / (listed * groups * TILE * TILE))

    first, second = total_of(0), total_of(groups)
    a = [first[0, k] for k in range(5)]
    b = [second[0, k] for k in range(5)]
    energies = [
        (a[3], a[3], a[4]),
        (a[0], a[1], a[2]),
        (b[0], b[1], b[2]),
        (b[3], b[4], b[4]),
    ]
    up = [e[2] - e[1] for e in energies]
    down = [e[0] - e[1] for e in energies]
    prof = [0.0, up[0], up[0] + up[1], up[0] + up[1] + up[2]]
    changes = [up[n] + down[n + 1] for n in range(3)]
    for n in range(2):
        for k in range(3):
            energy_ref[n, k] = jnp.where(win == 0, energies[n][k], energies[2 + n][k])
        profile_ref[n] = jnp.where(win == 0, prof[n], prof[2 + n])
        low, has = lows[n]
        change = jnp.where(low <= 0, changes[0], jnp.where(low == 1, changes[1], changes[2]))
        margin_ref[n] = jnp.where(has, logs[n] - beta[0] * change, 0.0)
    pltpu.make_async_copy(
        parts.at[pl.ds(0, wins * groups - 1)], parts.at[pl.ds(0, wins * groups - 1)], sum_send
    ).wait()


def per_device(atom_table, row_blocks, col_blocks, lambdas, inverse_temp, parity, thresholds):
    wins = lax.axis_size("win")
    groups = lax.axis_size("grp")
    own = atom_table.shape[2] // TILE
    listed = row_blocks.shape[1]
    lines = groups // LINE
    per_line = LINE * SLOTS
    hbm = pl.BlockSpec(memory_space=pl.ANY)
    smem = pl.BlockSpec(memory_space=pltpu.SMEM)
    f32, i32 = jnp.float32, jnp.int32
    results = pl.pallas_call(
        functools.partial(kernel, (wins, groups, own, listed)),
        out_shape=(
            jax.ShapeDtypeStruct((2, 3), f32),
            jax.ShapeDtypeStruct((2,), f32),
            jax.ShapeDtypeStruct((2,), f32),
        ),
        in_specs=[hbm] * 7,
        out_specs=(smem, smem, smem),
        scratch_shapes=[
            pltpu.VMEM((FIELDS, 2, own * TILE), f32),
            pltpu.SMEM((2, listed), i32),
            pltpu.SMEM((2, listed), i32),
            pltpu.VMEM((2, listed), i32),
            pltpu.SMEM((4,), f32),
            pltpu.SMEM((1,), f32),
            pltpu.SMEM((1,), i32),
            pltpu.SMEM((4,), i32),
            pltpu.VMEM((LINE * own, FIELDS, TILE), f32),
            pltpu.VMEM((LINE * own, FIELDS, TILE), f32),
            pltpu.VMEM((2, own, FIELDS + 3, TILE, TILE), f32),
            pltpu.VMEM((lines, 1, TILE), i32),
            pltpu.SMEM((lines, 1, TILE), i32),
            pltpu.VMEM((2, TILE), i32),
            pltpu.SMEM((2, TILE), i32),
            pltpu.VMEM((lines - 1, per_line, FIELDS, TILE), f32),
            pltpu.VMEM((lines - 1, per_line, FIELDS, TILE), f32),
            pltpu.VMEM((lines * per_line, FIELDS, TILE), f32),
            pltpu.VMEM((lines * per_line, FIELDS, TILE), f32),
            pltpu.VMEM((1, TILE), f32),
            pltpu.VMEM((wins * groups, 1, TILE), f32),
            pltpu.SemaphoreType.DMA((10,)),
            pltpu.SemaphoreType.DMA((2,)),
            pltpu.SemaphoreType.DMA((2,)),
            pltpu.SemaphoreType.DMA,
            pltpu.SemaphoreType.DMA((lines,)),
            pltpu.SemaphoreType.DMA((2,)),
            pltpu.SemaphoreType.DMA((2,)),
            pltpu.SemaphoreType.DMA,
            pltpu.SemaphoreType.DMA,
        ],
        compiler_params=pltpu.CompilerParams(collective_id=0, has_side_effects=True),
        name="exchange",
    )(
        jnp.transpose(atom_table, (1, 0, 2)),
        row_blocks,
        col_blocks,
        lambdas,
        inverse_temp,
        parity,
        thresholds,
    )

    def hand_over(*refs):
        copies = [pltpu.make_async_copy(refs[n], refs[3 + n], refs[6].at[n]) for n in range(3)]
        for copy in copies:
            copy.start()
        for copy in copies:
            copy.wait()

    return pl.pallas_call(
        hand_over,
        out_shape=tuple(jax.ShapeDtypeStruct(r.shape, r.dtype) for r in results),
        in_specs=[hbm] * 3,
        out_specs=(hbm,) * 3,
        scratch_shapes=[pltpu.SemaphoreType.DMA((3,))],
        name="hand_over",
    )(*results)


def solution(mesh):
    return jax.shard_map(
        per_device,
        mesh=mesh,
        in_specs=(P("win", None, "grp"), P("win", "grp"), P("win", "grp"), P(), P(), P(), P()),
        out_specs=(P("win", None), P("win"), P("win")),
        check_vma=False,
    )
```

```python
import functools

import jax
import jax.numpy as jnp
from jax import lax
from jax.experimental import pallas as pl
from jax.experimental.pallas import tpu as pltpu
from jax.sharding import PartitionSpec as P

TILE = 128
SUB = 8
FIELDS = 6
LINE = 4
SLOTS = 2
MESH = pl.DeviceIdType.MESH


def hops(offset):
    return min(offset, LINE - offset)


def kernel(
    sizes,
    table_hbm,
    rows_hbm,
    cols_hbm,
    lam_hbm,
    beta_hbm,
    parity_hbm,
    thresh_hbm,
    energy_ref,
    margin_ref,
    profile_ref,
    table,
    rows,
    cols_s,
    cols,
    lam,
    beta,
    parity,
    thresh,
    line_inner,
    line_edge,
    rot,
    req,
    asked,
    pos,
    where_s,
    send_inner,
    send_edge,
    col_inner,
    col_edge,
    part,
    parts,
    local_sem,
    line_send,
    line_recv,
    req_send,
    req_recv,
    rep_send,
    rep_recv,
    sum_send,
    sum_recv,
):
    wins, groups, own, listed = sizes
    lines = groups // LINE
    per_line = LINE * SLOTS
    win = lax.axis_index("win")
    me = lax.axis_index("grp")
    my_line = me // LINE
    my_x = lax.rem(me, LINE)
    my_y = lax.rem(my_line, LINE)
    my_z = my_line // LINE
    near = sorted(range(1, lines), key=lambda s: hops(s // LINE) + hops(s % LINE))
    inner = 1 - win
    edge = win
    line_buf = (line_inner, line_edge)
    send_buf = (send_inner, send_edge)
    col_buf = (col_inner, col_edge)

    def plane(step):
        return lax.rem(my_z + step // LINE, LINE) * LINE + lax.rem(my_y + step % LINE, LINE)

    barrier = pltpu.get_barrier_semaphore()

    local = [
        pltpu.make_async_copy(src, dst, local_sem.at[number])
        for number, (src, dst) in enumerate(
            [
                (cols_hbm, cols),
                (table_hbm, table),
                (rows_hbm, rows),
                (cols_hbm, cols_s),
                (lam_hbm, lam),
                (beta_hbm, beta),
                (parity_hbm, parity),
                (thresh_hbm, thresh),
            ]
        )
    ]
    for copy in local:
        copy.start()

    for step in reversed(near):
        pl.semaphore_signal(
            barrier, inc=1, device_id=(win, plane(step) * LINE + my_x), device_id_type=MESH
        )
    for step in range(1, LINE):
        pl.semaphore_signal(
            barrier,
            inc=1,
            device_id=(win, my_line * LINE + lax.rem(my_x + step, LINE)),
            device_id_type=MESH,
        )
    pl.semaphore_signal(barrier, inc=1, device_id=(1 - win, me), device_id_type=MESH)

    local[0].wait()
    col_pair = cols[...]
    iota_line = lax.broadcasted_iota(jnp.int32, (lines, listed), 0)
    before = (
        lax.broadcasted_iota(jnp.int32, (listed, listed), 0)
        < lax.broadcasted_iota(jnp.int32, (listed, listed), 1)
    ).astype(jnp.float32)
    slot_iota = lax.broadcasted_iota(jnp.int32, (TILE, listed), 0)
    asks = jnp.zeros((lines, TILE), jnp.float32)
    for order, number in enumerate((inner, edge)):
        ids = jnp.where(number == 0, col_pair[0:1], col_pair[1:2])
        line_ids = jnp.zeros_like(ids)
        for bound in range(1, lines):
            line_ids += (ids >= bound * LINE * own).astype(jnp.int32)
        within = (ids - line_ids * (LINE * own)).astype(jnp.float32)
        hot = (line_ids == iota_line).astype(jnp.float32)
        earlier = jnp.dot(hot, before, preferred_element_type=jnp.float32)
        rank = jnp.sum(hot * earlier, axis=0, keepdims=True).astype(jnp.int32)
        place = line_ids * per_line + rank
        ranked = (rank + order * per_line == slot_iota).astype(jnp.float32)
        asks += lax.dot_general(
            hot * within, ranked, (((1,), (1,)), ((), ())), preferred_element_type=jnp.float32
        )
        pos[order : order + 1, :listed] = place
    asks = asks.astype(jnp.int32)
    for line in range(lines):
        req[line] = asks[line : line + 1]
    to_scalar = pltpu.make_async_copy(pos, where_s, local_sem.at[8])
    to_scalar.start()

    local[1].wait()
    for order, number in enumerate((inner, edge)):
        for field in range(FIELDS):
            pair = table[field]
            row = jnp.where(number == 0, pair[0:1], pair[1:2])
            if field == 5:
                row = 1.0 / row
            for block in range(own):
                line_buf[order][my_x * own + block, field : field + 1, :] = row[
                    :, block * TILE : (block + 1) * TILE
                ]

    pl.semaphore_wait(barrier, lines + LINE - 1)

    def request(step):
        return pltpu.make_async_remote_copy(
            src_ref=req.at[plane(step)],
            dst_ref=asked.at[my_line],
            send_sem=req_send,
            recv_sem=req_recv.at[my_line],
            device_id=(win, plane(step) * LINE + my_x),
            device_id_type=MESH,
        )

    for step in reversed(near):
        request(step).start()
    own_request = pltpu.make_async_copy(req.at[my_line], asked.at[my_line], local_sem.at[9])
    own_request.start()

    def share(order, step):
        return pltpu.make_async_remote_copy(
            src_ref=line_buf[order].at[pl.ds(my_x * own, own)],
            dst_ref=line_buf[order].at[pl.ds(my_x * own, own)],
            send_sem=line_send.at[order],
            recv_sem=line_recv.at[order],
            device_id=(win, my_line * LINE + lax.rem(my_x + step, LINE)),
            device_id_type=MESH,
        )

    for step in (2, 1, 3):
        share(0, step).start()

    for copy in local[2:]:
        copy.wait()

    lam_sets = [[lam[win + k] for k in range(3)], [lam[2 * win + k] for k in range(2)]]

    def rotate(order):
        def turn(number, carry):
            block = line_buf[order][my_x * own + number]
            root = 2.0 * jnp.sqrt(block[4:5])
            scale = 1.0 / root
            turned = [
                block[0:1],
                block[1:2],
                block[2:3],
                block[3:4],
                root,
                block[5:6] * block[5:6] * block[5:6] * scale,
                scale,
            ]
            for field, row in enumerate(turned):
                row = jnp.broadcast_to(row, (SUB, TILE))
                for tile in range(TILE // SUB):
                    span = slice(tile * SUB, (tile + 1) * SUB)
                    value = pltpu.roll(row, tile * SUB, 1, stride=1, stride_axis=0)
                    if field < FIELDS:
                        rot[order, number, field, span, :] = value
                    else:
                        for k, l in enumerate(lam_sets[order]):
                            rot[order, number, field + k, span, :] = value * (1.0 - 0.5 * l)
            return carry

        lax.fori_loop(0, own, turn, 0)


    to_scalar.wait()

    own_request.wait()

    def reply(order, step):
        return pltpu.make_async_remote_copy(
            src_ref=send_buf[order].at[step - 1],
            dst_ref=col_buf[order].at[pl.ds(my_line * per_line, per_line)],
            send_sem=rep_send.at[order],
            recv_sem=rep_recv.at[order],
            device_id=(win, plane(step) * LINE + my_x),
            device_id_type=MESH,
        )

    for step in near:
        pltpu.make_async_copy(asked.at[0], asked.at[0], req_recv.at[plane(step)]).wait()
    for order in range(2):
        pltpu.make_async_copy(
            line_buf[order].at[pl.ds(0, own * (LINE - 1))],
            line_buf[order].at[pl.ds(0, own * (LINE - 1))],
            line_recv.at[order],
        ).wait()

        for step in reversed(near):
            peer = plane(step)
            for slot in range(per_line):
                wanted = jnp.clip(asked[peer, 0, order * per_line + slot], 0, LINE * own - 1)
                send_buf[order][step - 1, slot] = line_buf[order][wanted]
            if order == 0:
                reply(order, step).start()
        if order == 0:
            for step in (2, 1, 3):
                share(1, step).start()
        for slot in range(per_line):
            wanted = jnp.clip(asked[my_line, 0, order * per_line + slot], 0, LINE * own - 1)
            col_buf[order][my_line * per_line + slot] = line_buf[order][wanted]
        if order == 0:
            rotate(0)
            rotate(1)

    first_sub = lax.broadcasted_iota(jnp.int32, (SUB, TILE), 0) == 0
    lane = lax.broadcasted_iota(jnp.int32, (1, TILE), 1)
    out_row = jnp.zeros((1, TILE), jnp.float32)
    count = 0
    for order, number in enumerate((inner, edge)):
        pltpu.make_async_copy(
            col_buf[order].at[pl.ds(0, (lines - 1) * per_line)],
            col_buf[order].at[pl.ds(0, (lines - 1) * per_line)],
            rep_recv.at[order],
        ).wait()
        if order == 0:

            for step in reversed(near):
                reply(1, step).start()
        lams = lam_sets[order]
        soft = [jnp.full((SUB, TILE), 2.0 - l, jnp.float32) for l in lams]

        def pair(p, totals, order=order, number=number, soft=soft):
            row_id = rows[number, p]
            local_row = jnp.clip(row_id - me * own, 0, own - 1)
            same = row_id == cols_s[number, p]
            drop = jnp.where(same, 0.0, 1.0)
            keep = jnp.where(first_sub, drop, 1.0)
            place = jnp.clip(where_s[order, p], 0, lines * per_line - 1)
            tile = col_buf[order][place]
            xj, yj, zj, qj, ej, sj = [
                jnp.broadcast_to(tile[f : f + 1], (SUB, TILE)) for f in range(FIELDS)
            ]
            disp = [jnp.zeros((SUB, TILE), jnp.float32) for _ in soft]
            coul = [jnp.zeros((SUB, TILE), jnp.float32) for _ in soft]
            for t in range(TILE // SUB):
                span = slice(t * SUB, (t + 1) * SUB)
                dx = rot[order, local_row, 0, span, :] - xj
                dy = rot[order, local_row, 1, span, :] - yj
                dz = rot[order, local_row, 2, span, :] - zj
                qi = rot[order, local_row, 3, span, :]
                gi = rot[order, local_row, 4, span, :]
                ai = rot[order, local_row, 5, span, :]
                r2 = dx * dx + dy * dy + dz * dz
                u = r2 * sj
                v = u * u * u * ai
                if t == 0:
                    qi = qi * keep
                for k in range(len(soft)):
                    w = 1.0 / (rot[order, local_row, FIELDS + k, span, :] + v)
                    g = w * (w - gi)
                    disp[k] += g * keep if t == 0 else g
                    coul[k] += qi * lax.rsqrt(r2 + soft[k])
            return tuple(
                total + ej * d + qj * c for total, d, c in zip(totals, disp, coul)
            )

        zero = jnp.zeros((SUB, TILE), jnp.float32)
        totals = lax.fori_loop(0, listed, pair, tuple(zero for _ in lams), unroll=8)
        for total, l in zip(totals, lams):
            out_row = jnp.where(lane == count, jnp.sum(jnp.sum(total, axis=0, keepdims=True), axis=1, keepdims=True) * l, out_row)
            count += 1

    flat = win * groups + me
    part[...] = out_row
    parts[flat] = out_row

    def tell(target_win, target):
        return pltpu.make_async_remote_copy(
            src_ref=part,
            dst_ref=parts.at[flat],
            send_sem=sum_send,
            recv_sem=sum_recv,
            device_id=(target_win, target),
            device_id_type=MESH,
        )

    def away(step):
        return hops(step // (LINE * LINE)) + hops(step // LINE % LINE) + hops(step % LINE)

    for step in sorted(range(groups), key=away, reverse=True):
        other = plane(step // LINE) * LINE + lax.rem(my_x + step % LINE, LINE)
        tell(1 - win, other).start()
        if step:
            tell(win, other).start()

    pltpu.make_async_copy(asked.at[pl.ds(0, lines - 1)], asked.at[pl.ds(0, lines - 1)], req_send).wait()
    for order in range(2):
        pltpu.make_async_copy(
            line_buf[order].at[pl.ds(0, own * (LINE - 1))],
            line_buf[order].at[pl.ds(0, own * (LINE - 1))],
            line_send.at[order],
        ).wait()
        pltpu.make_async_copy(send_buf[order], send_buf[order], rep_send.at[order]).wait()

    par = parity[0]
    windows = 4
    firsts = [wins * win, wins * win + 1]
    even = lax.rem(par, 2) == 0

    everyone = pltpu.make_async_copy(
        parts.at[pl.ds(0, wins * groups - 1)], parts.at[pl.ds(0, wins * groups - 1)], sum_recv
    )
    lows = []
    logs = []
    for w in firsts:
        same_par = lax.rem(w, 2) == lax.rem(par, 2)
        low = jnp.where(same_par, w, w - 1)
        has = (low >= 0) & (low + 1 < windows)
        safe = jnp.clip(low, 0, windows - 1)
        draw = ((thresh[safe] + par) & 1073741823) + 1
        share_of = jnp.full((SUB, TILE), draw, jnp.int32).astype(jnp.float32) / 1073741824.0
        logs.append(-jnp.log(share_of)[0, 0])
        lows.append((low, has))
    everyone.wait()

    def total_of(start):
        chains = [parts[start + k] for k in range(8)]
        for n in range(8, groups):
            chains[n % 8] = chains[n % 8] + parts[start + n]
        while len(chains) > 1:
            chains = [chains[2 * n] + chains[2 * n + 1] for n in range(len(chains) // 2)]
        return chains[0] * (1.0 / (listed * groups * TILE * TILE))

    first, second = total_of(0), total_of(groups)
    a = [first[0, k] for k in range(5)]
    b = [second[0, k] for k in range(5)]
    energies = [
        (a[3], a[3], a[4]),
        (a[0], a[1], a[2]),
        (b[0], b[1], b[2]),
        (b[3], b[4], b[4]),
    ]
    up = [e[2] - e[1] for e in energies]
    down = [e[0] - e[1] for e in energies]
    prof = [0.0, up[0], up[0] + up[1], up[0] + up[1] + up[2]]
    changes = [up[n] + down[n + 1] for n in range(3)]
    for n in range(2):
        for k in range(3):
            energy_ref[n, k] = jnp.where(win == 0, energies[n][k], energies[2 + n][k])
        profile_ref[n] = jnp.where(win == 0, prof[n], prof[2 + n])
        low, has = lows[n]
        change = jnp.where(low <= 0, changes[0], jnp.where(low == 1, changes[1], changes[2]))
        margin_ref[n] = jnp.where(has, logs[n] - beta[0] * change, 0.0)
    pltpu.make_async_copy(
        parts.at[pl.ds(0, wins * groups - 1)], parts.at[pl.ds(0, wins * groups - 1)], sum_send
    ).wait()


def per_device(atom_table, row_blocks, col_blocks, lambdas, inverse_temp, parity, thresholds):
    wins = lax.axis_size("win")
    groups = lax.axis_size("grp")
    own = atom_table.shape[2] // TILE
    listed = row_blocks.shape[1]
    lines = groups // LINE
    per_line = LINE * SLOTS
    hbm = pl.BlockSpec(memory_space=pl.ANY)
    smem = pl.BlockSpec(memory_space=pltpu.SMEM)
    f32, i32 = jnp.float32, jnp.int32
    results = pl.pallas_call(
        functools.partial(kernel, (wins, groups, own, listed)),
        out_shape=(
            jax.ShapeDtypeStruct((2, 3), f32),
            jax.ShapeDtypeStruct((2,), f32),
            jax.ShapeDtypeStruct((2,), f32),
        ),
        in_specs=[hbm] * 7,
        out_specs=(smem, smem, smem),
        scratch_shapes=[
            pltpu.VMEM((FIELDS, 2, own * TILE), f32),
            pltpu.SMEM((2, listed), i32),
            pltpu.SMEM((2, listed), i32),
            pltpu.VMEM((2, listed), i32),
            pltpu.SMEM((4,), f32),
            pltpu.SMEM((1,), f32),
            pltpu.SMEM((1,), i32),
            pltpu.SMEM((4,), i32),
            pltpu.VMEM((LINE * own, FIELDS, TILE), f32),
            pltpu.VMEM((LINE * own, FIELDS, TILE), f32),
            pltpu.VMEM((2, own, FIELDS + 3, TILE, TILE), f32),
            pltpu.VMEM((lines, 1, TILE), i32),
            pltpu.SMEM((lines, 1, TILE), i32),
            pltpu.VMEM((2, TILE), i32),
            pltpu.SMEM((2, TILE), i32),
            pltpu.VMEM((lines - 1, per_line, FIELDS, TILE), f32),
            pltpu.VMEM((lines - 1, per_line, FIELDS, TILE), f32),
            pltpu.VMEM((lines * per_line, FIELDS, TILE), f32),
            pltpu.VMEM((lines * per_line, FIELDS, TILE), f32),
            pltpu.VMEM((1, TILE), f32),
            pltpu.VMEM((wins * groups, 1, TILE), f32),
            pltpu.SemaphoreType.DMA((10,)),
            pltpu.SemaphoreType.DMA((2,)),
            pltpu.SemaphoreType.DMA((2,)),
            pltpu.SemaphoreType.DMA,
            pltpu.SemaphoreType.DMA((lines,)),
            pltpu.SemaphoreType.DMA((2,)),
            pltpu.SemaphoreType.DMA((2,)),
            pltpu.SemaphoreType.DMA,
            pltpu.SemaphoreType.DMA,
        ],
        compiler_params=pltpu.CompilerParams(collective_id=0, has_side_effects=True),
        name="exchange",
    )(
        jnp.transpose(atom_table, (1, 0, 2)),
        row_blocks,
        col_blocks,
        lambdas,
        inverse_temp,
        parity,
        thresholds,
    )

    def hand_over(*refs):
        copies = [pltpu.make_async_copy(refs[n], refs[3 + n], refs[6].at[n]) for n in range(3)]
        for copy in copies:
            copy.start()
        for copy in copies:
            copy.wait()

    return pl.pallas_call(
        hand_over,
        out_shape=tuple(jax.ShapeDtypeStruct(r.shape, r.dtype) for r in results),
        in_specs=[hbm] * 3,
        out_specs=(hbm,) * 3,
        scratch_shapes=[pltpu.SemaphoreType.DMA((3,))],
        name="hand_over",
    )(*results)


def solution(mesh):
    return jax.shard_map(
        per_device,
        mesh=mesh,
        in_specs=(P("win", None, "grp"), P("win", "grp"), P("win", "grp"), P(), P(), P(), P()),
        out_specs=(P("win", None), P("win"), P("win")),
        check_vma=False,
    )
```
